32 devices in a mesh: angle: 4 (over z), pos: 8 (over y, x, core).
Axes of the slice: x: 2, y: 2, z: 4, core: 2. Of those that a mesh axis runs over, the one named last changes fastest.
Arguments:
- amplitude: float32 [4, 32, 128, 128], P('angle', 'pos'), may hold values from 0 to 2.5
- offsets: int32 [4, 32, 2], P('angle', 'pos'), may hold values from 0 to 896, as said below
- probe_field: float32 [2, 128, 128], replicated, may hold values from -5 to 5
- object_field: float32 [4, 2, 1024, 1024], P('angle', None, 'pos'), may hold values from -5 to 5
- interp_index: int32 [4, 2, 1024], replicated, may hold values from 0 to 1022
- interp_weight: float32 [4, 2, 1024], replicated, may hold values from 0 to 1
Outputs:
- new_object: float32 [4, 2, 1024, 1024], P('angle', None, 'pos')
- new_probe: float32 [2, 128, 128], replicated
- recon: float32 [8, 128, 2, 1024], P('pos', 'angle')
The draws below stay inside these ranges and needn't reach their ends.
Inputs may be any that keep to these rules, and one draw needn't show every extreme that they name: For position j, offsets[a, j, 0] = max(0, min(896, (j // 4) * 128 - 128 // 2 + u)) with 0 <= u < 128; offsets[a, j, 1] lies in 0 to 896.
All inputs are finite; a program needn't handle non-finite values.
Results may differ from the reference program's by a relative error of at most 0.00007.
Values sent between devices are 32-bit elements; how exact they have to be, the bound alone decides.
A program may use at most 64 MiB of HBM per device.

```python
import math
import jax
import jax.numpy as jnp
from jax import lax

NOBJ = 1024
PATCH = 128
POS_DEV = 4
ZWIN = 2
ANGLES = 4
POSITIONS = 32
BAND = 128
N_POS = 8


def draw_offsets(key, part):
    key_rows = jax.random.fold_in(key, 11)
    key_cols = jax.random.fold_in(key, 12)
    owners = jnp.arange(POSITIONS, dtype=jnp.int32) // POS_DEV
    base = owners * BAND - PATCH // 2
    shifts = jax.random.randint(key_rows, (ANGLES, POSITIONS), 0, BAND, dtype=jnp.int32)
    first_rows = jnp.clip(base[None, :] + shifts, 0, NOBJ - PATCH)
    first_cols = jax.random.randint(key_cols, (ANGLES, POSITIONS), 0, NOBJ - PATCH + 1, dtype=jnp.int32)
    return jnp.stack([first_rows, first_cols], axis=-1).astype(jnp.int32)


def with_ends(array, own_key, low, high):
    longest = array.shape.index(max(array.shape))
    spots = []
    for shift in (0, 1):
        where = [jax.random.randint(jax.random.fold_in(own_key, axis), (), 0, length) for axis, length in enumerate(array.shape)]
        where[longest] = (where[longest] + shift) % array.shape[longest]
        spots.append(tuple(where))
    return array.at[spots[0]].set(low).at[spots[1]].set(high)


def block_scale(rng, dims, pieces, smallest, largest):
    factor_of, own = 1.0, jax.random.fold_in(rng, 6)
    for position, blocks in pieces:
        steps = jnp.exp(jax.random.uniform(jax.random.fold_in(own, position), (blocks,), jnp.float32, smallest / len(pieces), largest / len(pieces)))
        factor_of = factor_of * jnp.repeat(steps, dims[position] // blocks).reshape([-1 if axis == position else 1 for axis in range(len(dims))])
    return factor_of


def bell_draw(key, extent, scale, bound, split=(), kind=jnp.bfloat16):
    values = jax.random.normal(key, extent, jnp.float32) * scale
    if len(split) > 0:
        values = block_scale(key, extent, split, -0.22, 0.18) * values
    return jnp.clip(values, min=-bound, max=bound).astype(kind)


def setup_inputs(seed: int = 0) -> dict:
    seeds = jax.random.split(jax.random.key(seed), 7)
    amplitude = jnp.clip(2.5 * jax.random.uniform(seeds[0], (ANGLES, POSITIONS, PATCH, PATCH), jnp.float32) ** block_scale(seeds[0], (ANGLES, POSITIONS, PATCH, PATCH), ((0, 4), (1, 8)), -0.2, 0.2), 0.0, 2.5)
    offsets = draw_offsets(jax.random.fold_in(seeds[6], 71), 0)
    probe_field = bell_draw(seeds[2], (2, PATCH, PATCH), 0.8, 5.0, (), jnp.float32)
    object_field = bell_draw(seeds[3], (ANGLES, 2, NOBJ, NOBJ), 0.8, 5.0, ((0, 4), (2, 8)), jnp.float32)
    interp_index = with_ends(jax.random.randint(seeds[4], (ANGLES, ZWIN, NOBJ), 0, NOBJ - 1), jax.random.fold_in(seeds[4], 1), 0, (NOBJ - 1) - 1).astype(jnp.int32)
    interp_weight = jnp.clip(jax.random.uniform(seeds[5], (ANGLES, ZWIN, NOBJ), jnp.float32, 0.0, 1.0), 0.0, 1.0)
    return dict(amplitude=amplitude, offsets=offsets, probe_field=probe_field, object_field=object_field, interp_index=interp_index, interp_weight=interp_weight)


def ramp_matrix(length):
    ramp = jnp.arange(length, dtype=jnp.int32)
    differ = ramp[:, None] - ramp[None, :]
    spread = differ.astype(jnp.float32)
    squared = jnp.maximum(spread * spread, 1.0)
    odd_terms = jnp.where(differ % 2 != 0, -1.0 / (math.pi * math.pi * squared), 0.0)
    return jnp.where(differ == 0, 0.25, odd_terms).astype(jnp.float32)


def reference(amplitude, offsets, probe_field, object_field, interp_index, interp_weight):
    probe_c = lax.complex(probe_field[0], probe_field[1])
    power = probe_field[0] * probe_field[0] + probe_field[1] * probe_field[1]

    def one_angle(inputs):
        amps, places, layer = inputs
        field = lax.complex(layer[0], layer[1])

        def take_patch(place):
            return lax.dynamic_slice(field, (place[0], place[1]), (PATCH, PATCH))

        patches = jax.vmap(take_patch)(places)
        exit_wave = probe_c * patches
        spectrum = jnp.fft.fft2(exit_wave, norm="ortho")
        magnitude = jnp.abs(spectrum)
        fixed = spectrum * (amps / jnp.maximum(magnitude, 0.5))
        change = jnp.fft.ifft2(fixed, norm="ortho") - exit_wave
        contrib = jnp.conj(probe_c) * change
        numer = jnp.sum(jnp.conj(patches) * change, axis=0)
        denom = jnp.sum(jnp.real(patches) ** 2 + jnp.imag(patches) ** 2, axis=0)
        stacked = jnp.stack([jnp.real(contrib), jnp.imag(contrib), jnp.broadcast_to(power, contrib.shape)], axis=1)

        def accumulate(count, total):
            start = (jnp.int32(0), places[count, 0], places[count, 1])
            current = lax.dynamic_slice(total, start, (3, PATCH, PATCH))
            return lax.dynamic_update_slice(total, current + stacked[count], start)

        total = lax.fori_loop(0, POSITIONS, accumulate, jnp.zeros((3, NOBJ, NOBJ), jnp.float32))
        updated = layer + total[:2] / (total[2] + 1.0)
        return updated, jnp.stack([jnp.real(numer), jnp.imag(numer)]), denom

    new_object, numers, denoms = lax.map(one_angle, (amplitude, offsets, object_field))
    new_probe = probe_field + jnp.sum(numers, axis=0) / (jnp.sum(denoms, axis=0) + 1.0)
    sinogram = jnp.transpose(new_object[:, 1], (1, 0, 2))
    filtered = jnp.dot(sinogram.reshape(NOBJ * ANGLES, NOBJ), ramp_matrix(NOBJ), precision=lax.Precision.HIGHEST)
    filtered = jnp.moveaxis(filtered.reshape(NOBJ, ANGLES, NOBJ), 1, 0)

    def project_back(total, inputs):
        rows_angle, index_angle, weight_angle = inputs
        lower = jnp.take(rows_angle, index_angle, axis=1)
        upper = jnp.take(rows_angle, index_angle + 1, axis=1)
        return total + (1.0 - weight_angle) * lower + weight_angle * upper, None

    total, unused = lax.scan(project_back, jnp.zeros((NOBJ, ZWIN * NOBJ), jnp.float32),
                             (filtered, interp_index.reshape(ANGLES, ZWIN * NOBJ), interp_weight.reshape(ANGLES, ZWIN * NOBJ)))
    recon = (total * (math.pi / ANGLES)).reshape(N_POS, NOBJ // N_POS, ZWIN, NOBJ)
    return new_object, new_probe, recon
```

```python
import functools
import math

import jax
import jax.numpy as jnp
import numpy as np
from jax import lax
from jax.experimental import pallas as pl
from jax.experimental.pallas import tpu as pltpu
from jax.sharding import PartitionSpec as P

MESH = pl.DeviceIdType.MESH
VMEM = pltpu.VMEM
BIG = 60 * 1024 * 1024


def split_const(table):
    high = jnp.asarray(table, jnp.float32).astype(jnp.bfloat16)
    low = (jnp.asarray(table, jnp.float32) - high.astype(jnp.float32)).astype(jnp.bfloat16)
    return high, low


def dft_blocks(length):
    ramp = np.arange(length)
    theta = (ramp[:, None] * ramp[None, :] % length) * (2.0 * math.pi / length)
    real = np.cos(theta) / math.sqrt(length)
    imag = -np.sin(theta) / math.sqrt(length)
    left = np.block([[real, -imag], [imag, real]])
    right = np.block([[real, imag], [-imag, real]])
    return np.asarray(left, np.float32), np.asarray(right, np.float32)


def halves(value):
    high = value.astype(jnp.bfloat16)
    return high, (value - high.astype(jnp.float32)).astype(jnp.bfloat16)


def mm(a, b):
    return jnp.dot(a, b, preferred_element_type=jnp.float32)


def left3(table_high, table_low, value):
    high, low = halves(value)
    return mm(table_high, high) + mm(table_high, low) + mm(table_low, high)


def right3(value, table_high, table_low):
    high, low = halves(value)
    return mm(high, table_high) + mm(low, table_high) + mm(high, table_low)


def remote(src, dst, send, recv, axis, target):
    return pltpu.make_async_remote_copy(
        src_ref=src, dst_ref=dst, send_sem=send, recv_sem=recv,
        device_id={axis: target}, device_id_type=MESH,
    )


def patch_kernel(n_pos, row_at, obj, offs, amp, probe, ah, al, bh, bl,
                 grad, from_above, from_below, offs_near, numden,
                 ext, q, psi, local_sem, send_sem, recv_sem):
    me = lax.axis_index("pos")
    up, down = lax.rem(me + n_pos - 1, n_pos), lax.rem(me + 1, n_pos)
    band = obj.shape[2]
    width = obj.shape[3]
    patch = probe.shape[1]
    half = patch // 2
    count = amp.shape[0]
    inner = pltpu.make_async_copy(obj.at[0], ext.at[:, pl.ds(half, band), :], local_sem.at[0])
    inner.start()
    barrier = pltpu.get_barrier_semaphore()
    for target in (up, down):
        pl.semaphore_signal(barrier, inc=1, device_id={"pos": target}, device_id_type=MESH)
    pl.semaphore_wait(barrier, 2)
    first = [
        remote(obj.at[0, :, pl.ds(band - half, half), :], ext.at[:, pl.ds(0, half), :],
               send_sem.at[0], recv_sem.at[0], "pos", down),
        remote(obj.at[0, :, pl.ds(0, half), :], ext.at[:, pl.ds(half + band, half), :],
               send_sem.at[1], recv_sem.at[1], "pos", up),
        remote(offs, offs_near.at[0], send_sem.at[2], recv_sem.at[2], "pos", down),
        remote(offs, offs_near.at[1], send_sem.at[3], recv_sem.at[3], "pos", up),
    ]
    for copy in first:
        copy.start()
    p_re, p_im = probe[0], probe[1]
    wide_at = lax.broadcasted_iota(jnp.int32, (width, count * patch), 0)
    pick_cols = (wide_at == offs[0:1, :]).astype(jnp.bfloat16)
    tall_at = lax.broadcasted_iota(jnp.int32, (patch, band + patch), 1)

    def choose(spans):
        parts = []
        for c in range(2):
            split = [halves(ext[c, span, :]) for span in spans]
            parts += [piece[0] for piece in split] + [piece[1] for piece in split]
        return mm(jnp.concatenate(parts, axis=0), pick_cols).astype(jnp.bfloat16)

    inner.wait()
    inside = choose((slice(half, half + band),))
    for copy in first:
        copy.wait()
    outer = choose((slice(0, half), slice(half + band, patch + band)))
    for j in range(count):
        pick_rows = (tall_at == row_at[j * patch:(j + 1) * patch, :]).astype(jnp.bfloat16)
        span = pl.ds(j * patch, patch)
        parts = []
        for k in range(4):
            parts += [outer[k * patch:k * patch + half, j * patch:(j + 1) * patch],
                      inside[k * band:(k + 1) * band, j * patch:(j + 1) * patch],
                      outer[k * patch + half:(k + 1) * patch, j * patch:(j + 1) * patch]]
        lines = [jnp.concatenate(parts[3 * k:3 * k + 3], axis=0) for k in range(4)]
        got = mm(pick_rows, jnp.concatenate(lines, axis=1))
        cut = [got[:, 2 * c * patch:(2 * c + 1) * patch] + got[:, (2 * c + 1) * patch:(2 * c + 2) * patch]
               for c in range(2)]
        q[0:patch, span] = cut[0]
        q[patch:, span] = cut[1]
        psi[0:patch, span] = p_re * cut[0] - p_im * cut[1]
        psi[patch:, span] = p_re * cut[1] + p_im * cut[0]
    mid = left3(ah[...], al[...], psi[...])
    rows = [
        jnp.concatenate(
            [mid[:patch, j * patch:(j + 1) * patch], mid[patch:, j * patch:(j + 1) * patch]], axis=1)
        for j in range(count)
    ]
    spec = right3(jnp.concatenate(rows, axis=0), bh[...], bl[...])
    fixed = []
    for j in range(count):
        s_re = spec[j * patch:(j + 1) * patch, :patch]
        s_im = spec[j * patch:(j + 1) * patch, patch:]
        factor = amp[j] / jnp.maximum(jnp.sqrt(s_re * s_re + s_im * s_im), 0.5)
        fixed.append(jnp.concatenate([factor * s_re, factor * s_im], axis=1))
    back = right3(jnp.concatenate(fixed, axis=0), ah[...], al[...])
    wide_re = jnp.concatenate([back[j * patch:(j + 1) * patch, :patch] for j in range(count)], axis=1)
    wide_im = jnp.concatenate([back[j * patch:(j + 1) * patch, patch:] for j in range(count)], axis=1)
    diff = left3(bh[...], bl[...], jnp.concatenate([wide_re, wide_im], axis=0)) - psi[...]
    n_re = jnp.zeros((patch, patch), jnp.float32)
    n_im = n_re
    den = n_re
    for j in range(count):
        lanes = slice(j * patch, (j + 1) * patch)
        d_re, d_im = diff[:patch, lanes], diff[patch:, lanes]
        g_re = p_re * d_re + p_im * d_im
        g_im = p_re * d_im - p_im * d_re
        for h in range(2):
            grad[h, 0, j] = g_re[h * half:(h + 1) * half]
            grad[h, 1, j] = g_im[h * half:(h + 1) * half]
        q_re, q_im = q[0:patch, lanes], q[patch:, lanes]
        n_re = n_re + (q_re * d_re + q_im * d_im)
        n_im = n_im + (q_re * d_im - q_im * d_re)
        den = den + (q_re * q_re + q_im * q_im)
    numden[0] = n_re
    numden[1] = n_im
    numden[2] = den
    second = [
        remote(grad.at[1], from_above, send_sem.at[4], recv_sem.at[4], "pos", down),
        remote(grad.at[0], from_below, send_sem.at[5], recv_sem.at[5], "pos", up),
    ]
    for copy in second:
        copy.start()
    for copy in second:
        copy.wait()


def merge_kernel(start_ref, own_ref, near_ref, obj, probe, grad, from_above, from_below,
                 out, acc):
    band = obj.shape[2]
    width = obj.shape[3]
    patch = probe.shape[1]
    half = patch // 2
    count = own_ref.shape[0]
    start = start_ref[0]
    acc[...] = jnp.zeros_like(acc)
    power = probe[0] * probe[0] + probe[1] * probe[1]
    last = acc.shape[1] - 8

    def place(planes, row, col):
        height = planes[0].shape[0]
        tile = jnp.minimum(col // 128, width // 128 - 2)
        base = pl.multiple_of(tile * 128, 128)
        shift = col - base
        top = pl.multiple_of(row // 8 * 8, 8)
        drop = row - top
        for c in range(3):
            tall = jnp.concatenate([planes[c], jnp.zeros((8, patch), jnp.float32)], axis=0)
            tall = pltpu.roll(tall, drop, 0)
            wide = jnp.concatenate([tall, jnp.zeros((height + 8, 128), jnp.float32)], axis=1)
            wide = pltpu.roll(wide, shift, 1)
            spot = (c, pl.ds(top, height + 8), pl.ds(base, 256))
            acc[spot] = acc[spot] + wide

    for j in range(count):
        planes = [jnp.concatenate([grad[0, c, j], grad[1, c, j]], axis=0) for c in range(2)]
        place(planes + [power], own_ref[j, 0] - start + patch, own_ref[j, 1])
    for side, ref in ((0, from_above), (1, from_below)):
        for j in range(count):
            row = near_ref[side, 1, j] - start + patch + (half if side == 0 else 0)
            col = near_ref[side, 0, j]

            @pl.when((row >= 0) & (row <= last - half))
            def _(side=side, ref=ref, j=j, row=row, col=col):
                part = power[half:] if side == 0 else power[:half]
                place([ref[0, j], ref[1, j], part], row, col)

    rows = pl.ds(patch, band)
    scale = acc[2, rows, :] + 1.0
    for c in range(2):
        out[0, c] = obj[0, c] + acc[c, rows, :] / scale


def final_kernel(n_ang, n_pos, new_obj, numden, probe, index, weight,
                 recon, newp,
                 sino, onehot, rh, rl, filt, rs, ag, piece,
                 local_sem, a2a_send, a2a_recv, rs_send, rs_recv, ag_send, ag_recv,
                 fin_send, fin_recv):
    me_a = lax.axis_index("angle")
    me_p = lax.axis_index("pos")
    ns = sino.shape[1]
    width = sino.shape[2]
    total = index.shape[1]
    pr = piece.shape[1]
    loads = [
        pltpu.make_async_copy(new_obj.at[0, 1, pl.ds(pl.multiple_of(me_a * ns, 8), ns), :],
                              sino.at[me_a], local_sem.at[0]),
    ]
    for copy in loads:
        copy.start()
    barrier = pltpu.get_barrier_semaphore()
    angle_peers = [lax.rem(me_a + d, n_ang) for d in range(1, n_ang)]
    pos_peers = [lax.rem(me_p + d, n_pos) for d in range(1, n_pos)]
    for peer in angle_peers:
        pl.semaphore_signal(barrier, inc=1, device_id={"angle": peer}, device_id_type=MESH)
    for peer in pos_peers:
        pl.semaphore_signal(barrier, inc=1, device_id={"pos": peer}, device_id_type=MESH)
    pl.semaphore_wait(barrier, n_ang + n_pos - 2)
    across = [
        remote(new_obj.at[0, 1, pl.ds(pl.multiple_of(peer * ns, 8), ns), :], sino.at[me_a],
               a2a_send.at[d], a2a_recv.at[d], "angle", peer)
        for d, peer in enumerate(angle_peers)
    ]
    for copy in across:
        copy.start()
    scatter = [
        remote(numden.at[:, pl.ds(pl.multiple_of(peer * pr, 8), pr), :], rs.at[d],
               rs_send.at[d], rs_recv.at[d], "pos", peer)
        for d, peer in enumerate(pos_peers)
    ]
    for copy in scatter:
        copy.start()

    chunk = 256
    bins = lax.broadcasted_iota(jnp.int32, (width, chunk), 0)

    def build(step, carry):
        a = step // (total // chunk)
        lanes = pl.ds(pl.multiple_of(lax.rem(step, total // chunk) * chunk, chunk), chunk)
        hit = bins == index[pl.ds(a, 1), lanes]
        onehot[a, :, lanes] = jnp.where(hit, 1.0, 0.0).astype(jnp.bfloat16)
        return carry

    lax.fori_loop(0, n_ang * (total // chunk), build, 0)

    tall = 64

    def ramp(step, carry):
        top = pl.multiple_of(step * tall, tall)
        shape = (tall, width)
        differ = lax.broadcasted_iota(jnp.int32, shape, 1) - (
            lax.broadcasted_iota(jnp.int32, shape, 0) + top)
        spread = differ.astype(jnp.float32)
        odd = -1.0 / (jnp.maximum(spread * spread, 1.0) * (math.pi * math.pi))
        value = jnp.where((differ & 1) == 1, odd, jnp.where(differ == 0, 0.25, 0.0))
        rh[pl.ds(top, tall), :], rl[pl.ds(top, tall), :] = halves(value)
        return carry

    lax.fori_loop(0, width // tall, ramp, 0)
    for copy in scatter:
        copy.wait()
    part = numden[:, pl.ds(pl.multiple_of(me_p * pr, 8), pr), :]
    for d in range(n_pos - 1):
        part = part + rs[d]
    ag[me_a] = part
    gather = [
        remote(ag.at[me_a], ag.at[me_a], ag_send.at[d], ag_recv.at[d], "angle", peer)
        for d, peer in enumerate(angle_peers)
    ]
    for copy in gather:
        copy.start()
    for copy in loads:
        copy.wait()
    for copy in across:
        copy.wait()

    rows = n_ang * ns
    high, low = halves(sino[...].reshape(rows, width))
    both = mm(jnp.concatenate([high, low], axis=0), rh[...])
    filtered = both[:rows] + both[rows:] + mm(high, rl[...])
    filt[...] = filtered.reshape(n_ang, ns, width)

    for copy in gather:
        copy.wait()
    whole = ag[0]
    for a in range(1, n_ang):
        whole = whole + ag[a]
    mine = pl.ds(pl.multiple_of(me_p * pr, 8), pr)
    for c in range(2):
        value = probe[c, mine, :] + whole[c] / (whole[2] + 1.0)
        piece[c] = value
        newp[c, mine, :] = value
    spread = [
        remote(piece, newp.at[:, mine, :], fin_send.at[d], fin_recv.at[d], "pos", peer)
        for d, peer in enumerate(pos_peers)
    ]
    for copy in spread:
        copy.start()

    recon[...] = jnp.zeros_like(recon)
    wide = 512

    def project(a, carry):
        lines = filt[a] * (math.pi / n_ang)
        high, low = halves(lines)
        next_high, next_low = halves(pltpu.roll(lines, width - 1, 1))
        stack = jnp.concatenate([high, low, next_high, next_low], axis=0)
        for n in range(total // wide):
            lanes = pl.ds(n * wide, wide)
            got = mm(stack, onehot[a, :, lanes])
            lower = got[:ns] + got[ns:2 * ns]
            upper = got[2 * ns:3 * ns] + got[3 * ns:]
            w = weight[pl.ds(a, 1), lanes]
            recon[:, lanes] += (1.0 - w) * lower + w * upper
        return carry

    lax.fori_loop(0, n_ang, project, 0)
    for copy in spread:
        copy.wait()


def on_device(n_ang, n_pos, amplitude, offsets, probe_field, object_field, interp_index, interp_weight):
    band = object_field.shape[2]
    width = object_field.shape[3]
    patch = probe_field.shape[1]
    half = patch // 2
    count = offsets.shape[1]
    f32, i32 = jnp.float32, jnp.int32
    start = lax.axis_index("pos").astype(i32) * band
    own = offsets[0]
    ramp = jnp.arange(patch, dtype=i32)[None, :]
    row_at = (own[:, :1] - (start - half) + ramp).reshape(count * patch, 1)
    lanes = (own[:, 1:] + ramp).reshape(1, count * patch)
    first_rows = (own[:, :1] + 0 * ramp).reshape(1, count * patch)
    padded = jnp.concatenate([lanes, first_rows, jnp.zeros((6, count * patch), i32)], axis=0)
    left, right = dft_blocks(patch)
    ah, al = split_const(left)
    bh, bl = split_const(right)
    vmem = pl.BlockSpec(memory_space=VMEM)
    smem = pl.BlockSpec(memory_space=pltpu.SMEM)
    hbm = pl.BlockSpec(memory_space=pl.ANY)
    sds = jax.ShapeDtypeStruct
    dma = pltpu.SemaphoreType.DMA
    half_shape = (2, count, half, patch)
    grad, from_above, from_below, near, numden = pl.pallas_call(
        functools.partial(patch_kernel, n_pos),
        out_shape=(
            sds((2,) + half_shape, f32), sds(half_shape, f32), sds(half_shape, f32),
            sds((2, 8, count * patch), i32), sds((3, patch, patch), f32),
        ),
        in_specs=[vmem, hbm] + [vmem] * 7,
        out_specs=(vmem,) * 5,
        scratch_shapes=[
            VMEM((2, band + patch, width), f32),
            VMEM((2 * patch, count * patch), f32),
            VMEM((2 * patch, count * patch), f32),
            dma((1,)), dma((6,)), dma((6,)),
        ],
        compiler_params=pltpu.CompilerParams(collective_id=0, has_side_effects=True),
        name="patches",
    )(row_at, object_field, padded, amplitude[0], probe_field, ah, al, bh, bl)
    new_object = pl.pallas_call(
        merge_kernel,
        out_shape=sds(object_field.shape, f32),
        in_specs=[smem] * 3 + [vmem] * 5,
        out_specs=vmem,
        scratch_shapes=[VMEM((3, band + 2 * patch + 8, width), f32)],
        name="merge",
    )(start[None], own, near[:, :2, ::patch], object_field, probe_field, grad, from_above, from_below)
    zwin = interp_index.shape[1]
    total = zwin * width
    ns = band // n_ang
    pr = patch // n_pos
    bf16 = jnp.bfloat16
    recon, new_probe = pl.pallas_call(
        functools.partial(final_kernel, n_ang, n_pos),
        out_shape=(sds((ns, total), f32), sds(probe_field.shape, f32)),
        in_specs=[hbm] + [vmem] * 4,
        out_specs=(vmem, vmem),
        scratch_shapes=[
            VMEM((n_ang, ns, width), f32),
            VMEM((n_ang, width, total), bf16),
            VMEM((width, width), bf16), VMEM((width, width), bf16),
            VMEM((n_ang, ns, width), f32),
            VMEM((n_pos - 1, 3, pr, patch), f32),
            VMEM((n_ang, 3, pr, patch), f32),
            VMEM((2, pr, patch), f32),
            dma((1,)),
            dma((n_ang - 1,)), dma((n_ang - 1,)),
            dma((n_pos - 1,)), dma((n_pos - 1,)),
            dma((n_ang - 1,)), dma((n_ang - 1,)),
            dma((n_pos - 1,)), dma((n_pos - 1,)),
        ],
        compiler_params=pltpu.CompilerParams(
            collective_id=1, has_side_effects=True, vmem_limit_bytes=BIG),
        name="final",
    )(new_object, numden, probe_field, interp_index.reshape(n_ang, total),
      interp_weight.reshape(n_ang, total))
    return new_object, new_probe, recon.reshape(1, ns, zwin, width)


def solution(mesh):
    placed = (
        P("angle", "pos", None, None),
        P("angle", "pos", None),
        P(),
        P("angle", None, "pos", None),
        P(),
        P(),
    )
    return jax.shard_map(
        functools.partial(on_device, mesh.shape["angle"], mesh.shape["pos"]),
        mesh=mesh,
        in_specs=placed,
        out_specs=(P("angle", None, "pos", None), P(), P("pos", "angle", None, None)),
        check_vma=False,
    )
```

```python
import functools
import math

import jax
import jax.numpy as jnp
import numpy as np
from jax import lax
from jax.experimental import pallas as pl
from jax.experimental.pallas import tpu as pltpu
from jax.sharding import PartitionSpec as P

MESH = pl.DeviceIdType.MESH
VMEM = pltpu.VMEM
BIG = 60 * 1024 * 1024


def split_const(table):
    high = jnp.asarray(table, jnp.float32).astype(jnp.bfloat16)
    low = (jnp.asarray(table, jnp.float32) - high.astype(jnp.float32)).astype(jnp.bfloat16)
    return high, low


def dft_blocks(length):
    ramp = np.arange(length)
    theta = (ramp[:, None] * ramp[None, :] % length) * (2.0 * math.pi / length)
    real = np.cos(theta) / math.sqrt(length)
    imag = -np.sin(theta) / math.sqrt(length)
    left = np.block([[real, -imag], [imag, real]])
    right = np.block([[real, imag], [-imag, real]])
    return np.asarray(left, np.float32), np.asarray(right, np.float32)


def halves(value):
    high = value.astype(jnp.bfloat16)
    return high, (value - high.astype(jnp.float32)).astype(jnp.bfloat16)


def mm(a, b):
    return jnp.dot(a, b, preferred_element_type=jnp.float32)


def left3(table_high, table_low, value):
    high, low = halves(value)
    return mm(table_high, high) + mm(table_high, low) + mm(table_low, high)


def right3(value, table_high, table_low):
    high, low = halves(value)
    return mm(high, table_high) + mm(low, table_high) + mm(high, table_low)


def remote(src, dst, send, recv, axis, target):
    return pltpu.make_async_remote_copy(
        src_ref=src, dst_ref=dst, send_sem=send, recv_sem=recv,
        device_id={axis: target}, device_id_type=MESH,
    )


def patch_kernel(n_pos, where_at, obj, offs, index, amp, probe, ah, al, bh, bl,
                 grad, from_above, from_below, offs_near, partial, onehot,
                 ext, table, numden, rs,
                 local_sem, table_sem, send_sem, recv_sem, rs_send, rs_recv):
    me = lax.axis_index("pos")
    up, down = lax.rem(me + n_pos - 1, n_pos), lax.rem(me + 1, n_pos)
    band = obj.shape[2]
    width = obj.shape[3]
    patch = probe.shape[1]
    half = patch // 2
    count = amp.shape[0]
    inner = pltpu.make_async_copy(obj.at[0], ext.at[:, pl.ds(half, band), :], local_sem.at[0])
    inner.start()
    barrier = pltpu.get_barrier_semaphore()
    pos_peers = [lax.rem(me + d, n_pos) for d in range(1, n_pos)]
    for target in pos_peers:
        pl.semaphore_signal(barrier, inc=1, device_id={"pos": target}, device_id_type=MESH)
    pl.semaphore_wait(barrier, n_pos - 1)
    first = [
        remote(obj.at[0, :, pl.ds(band - half, half), :], ext.at[:, pl.ds(0, half), :],
               send_sem.at[0], recv_sem.at[0], "pos", down),
        remote(obj.at[0, :, pl.ds(0, half), :], ext.at[:, pl.ds(half + band, half), :],
               send_sem.at[1], recv_sem.at[1], "pos", up),
        remote(offs, offs_near.at[0], send_sem.at[2], recv_sem.at[2], "pos", down),
        remote(offs, offs_near.at[1], send_sem.at[3], recv_sem.at[3], "pos", up),
    ]
    for copy in first:
        copy.start()
    p_re, p_im = probe[0], probe[1]
    wide_at = lax.broadcasted_iota(jnp.int32, (width, count * patch), 0)
    pick_cols = (wide_at == where_at[0:1, :]).astype(jnp.bfloat16)
    tall_at = lax.broadcasted_iota(jnp.int32, (patch, band + patch), 1)

    def choose(spans):
        parts = []
        for c in range(2):
            split = [halves(ext[c, span, :]) for span in spans]
            parts += [piece[0] for piece in split] + [piece[1] for piece in split]
        return mm(jnp.concatenate(parts, axis=0), pick_cols).astype(jnp.bfloat16)

    inner.wait()
    inside = choose((slice(half, half + band),))
    chunk = table.shape[2]
    per_row = width // chunk
    zwin = index.shape[1]
    steps = onehot.shape[0]
    bins = lax.broadcasted_iota(jnp.int32, (width, chunk), 0)

    def shipped(step, slot):
        return pltpu.make_async_copy(table.at[slot], onehot.at[step], table_sem.at[slot])

    def build(step, slot):
        a = step // (zwin * per_row)
        z = lax.rem(step // per_row, zwin)
        lanes = pl.ds(pl.multiple_of(lax.rem(step, per_row) * chunk, chunk), chunk)
        hit = bins == index[a, pl.ds(z, 1), lanes]
        table[slot] = jnp.where(hit, 1.0, 0.0).astype(jnp.bfloat16)
        shipped(step, slot).start()

    def build_pair(pair, carry):
        for slot in range(2):
            shipped(2 * pair + slot - 2, slot).wait()
            build(2 * pair + slot, slot)
        return carry

    for slot in range(2):
        build(jnp.int32(slot), slot)
    lax.fori_loop(1, steps // 2, build_pair, 0)
    for copy in first:
        copy.wait()
    outer = choose((slice(0, half), slice(half + band, patch + band)))
    n_re = jnp.zeros((patch, patch), jnp.float32)
    n_im = n_re
    den = n_re
    second = []
    size = 2 if count % 2 == 0 else count
    for g in range(count // size):
        group = range(g * size, (g + 1) * size)
        q_re, q_im, w_re, w_im = [], [], [], []
        for j in group:
            row_at = jnp.broadcast_to(where_at[1:2, j * patch:(j + 1) * patch], (patch, patch))
            row_at = jnp.transpose(row_at)[:, :1]
            pick_rows = (tall_at == row_at).astype(jnp.bfloat16)
            parts = []
            for k in range(4):
                parts += [outer[k * patch:k * patch + half, j * patch:(j + 1) * patch],
                          inside[k * band:(k + 1) * band, j * patch:(j + 1) * patch],
                          outer[k * patch + half:(k + 1) * patch, j * patch:(j + 1) * patch]]
            lines = [jnp.concatenate(parts[3 * k:3 * k + 3], axis=0) for k in range(4)]
            got = mm(pick_rows, jnp.concatenate(lines, axis=1))
            re = got[:, :patch] + got[:, patch:2 * patch]
            im = got[:, 2 * patch:3 * patch] + got[:, 3 * patch:]
            q_re.append(re)
            q_im.append(im)
            w_re.append(p_re * re - p_im * im)
            w_im.append(p_re * im + p_im * re)
        psi = jnp.concatenate([jnp.concatenate(w_re, axis=1), jnp.concatenate(w_im, axis=1)], axis=0)
        mid = left3(ah[...], al[...], psi)
        cells = [slice(n * patch, (n + 1) * patch) for n in range(size)]
        rows = [jnp.concatenate([mid[:patch, cell], mid[patch:, cell]], axis=1) for cell in cells]
        spec = right3(jnp.concatenate(rows, axis=0), bh[...], bl[...])
        fixed = []
        for j, cell in zip(group, cells):
            s_re = spec[cell, :patch]
            s_im = spec[cell, patch:]
            factor = amp[j] / jnp.maximum(jnp.sqrt(s_re * s_re + s_im * s_im), 0.5)
            fixed.append(jnp.concatenate([factor * s_re, factor * s_im], axis=1))
        back = right3(jnp.concatenate(fixed, axis=0), ah[...], al[...])
        wide_re = jnp.concatenate([back[cell, :patch] for cell in cells], axis=1)
        wide_im = jnp.concatenate([back[cell, patch:] for cell in cells], axis=1)
        diff = left3(bh[...], bl[...], jnp.concatenate([wide_re, wide_im], axis=0))
        diff = diff - psi
        for n, j in enumerate(group):
            d_re, d_im = diff[:patch, cells[n]], diff[patch:, cells[n]]
            g_re = p_re * d_re + p_im * d_im
            g_im = p_re * d_im - p_im * d_re
            for h in range(2):
                grad[h, j, 0] = g_re[h * half:(h + 1) * half]
                grad[h, j, 1] = g_im[h * half:(h + 1) * half]
            n_re = n_re + (q_re[n] * d_re + q_im[n] * d_im)
            n_im = n_im + (q_re[n] * d_im - q_im[n] * d_re)
            den = den + (q_re[n] * q_re[n] + q_im[n] * q_im[n])
        if g == count // size - 1:
            numden[0] = n_re
            numden[1] = n_im
            numden[2] = den
        span = pl.ds(g * size, size)
        sems = [4 + 2 * g, 5 + 2 * g]
        pair = [
            remote(grad.at[1, span], from_above.at[span], send_sem.at[sems[0]],
                   recv_sem.at[sems[0]], "pos", down),
            remote(grad.at[0, span], from_below.at[span], send_sem.at[sems[1]],
                   recv_sem.at[sems[1]], "pos", up),
        ]
        for copy in pair:
            copy.start()
        second += pair
    pr = patch // n_pos
    scatter = [
        remote(numden.at[:, pl.ds(pl.multiple_of(peer * pr, 8), pr), :], rs.at[d],
               rs_send.at[d], rs_recv.at[d], "pos", peer)
        for d, peer in enumerate(pos_peers)
    ]
    for copy in scatter:
        copy.start()
    for slot in range(2):
        shipped(steps - 2 + slot, slot).wait()
    for copy in scatter:
        copy.wait()
    part = numden[:, pl.ds(pl.multiple_of(me * pr, 8), pr), :]
    for d in range(n_pos - 1):
        part = part + rs[d]
    partial[...] = part
    for copy in second:
        copy.wait()


def merge_kernel(count, start_ref, own_ref, near_ref, obj, probe, grad, from_above, from_below,
                 out, acc):
    band = obj.shape[2]
    width = obj.shape[3]
    patch = probe.shape[1]
    half = patch // 2
    start = start_ref[0]
    acc[...] = jnp.zeros_like(acc)
    power = probe[0] * probe[0] + probe[1] * probe[1]
    last = acc.shape[1] - 8

    def place(planes, row, col):
        height = planes[0].shape[0]
        tile = jnp.minimum(col // 128, width // 128 - 2)
        base = pl.multiple_of(tile * 128, 128)
        shift = col - base
        top = pl.multiple_of(row // 8 * 8, 8)
        drop = row - top
        for c in range(3):
            tall = jnp.concatenate([planes[c], jnp.zeros((8, patch), jnp.float32)], axis=0)
            tall = pltpu.roll(tall, drop, 0)
            wide = jnp.concatenate([tall, jnp.zeros((height + 8, 128), jnp.float32)], axis=1)
            wide = pltpu.roll(wide, shift, 1)
            spot = (c, pl.ds(top, height + 8), pl.ds(base, 256))
            acc[spot] = acc[spot] + wide

    for j in range(count):
        planes = [jnp.concatenate([grad[0, j, c], grad[1, j, c]], axis=0) for c in range(2)]
        place(planes + [power], own_ref[0, 2 * j] - start + patch, own_ref[0, 2 * j + 1])
    for side, ref in ((0, from_above), (1, from_below)):
        for j in range(count):
            row = near_ref[side, 0, 2 * j] - start + patch + (half if side == 0 else 0)
            col = near_ref[side, 0, 2 * j + 1]

            @pl.when((row >= 0) & (row <= last - half))
            def _(side=side, ref=ref, j=j, row=row, col=col):
                part = power[half:] if side == 0 else power[:half]
                place([ref[j, 0], ref[j, 1], part], row, col)

    rows = pl.ds(patch, band)
    scale = acc[2, rows, :] + 1.0
    for c in range(2):
        out[0, c] = obj[0, c] + acc[c, rows, :] / scale


def final_kernel(n_ang, n_pos, new_obj, partial, weight, onehot,
                 recon, newp,
                 sino, tables, rh, rl, ag, piece,
                 local_sem, table_sem, a2a_send, a2a_recv, ag_send, ag_recv,
                 fin_send, fin_recv):
    me_a = lax.axis_index("angle")
    me_p = lax.axis_index("pos")
    ns = sino.shape[1]
    width = sino.shape[2]
    pr = piece.shape[1]
    chunk = tables.shape[2]
    per_row = width // chunk
    zwin = weight.shape[1]
    per_angle = zwin * per_row
    order = sorted(range(1, n_ang), key=lambda d: (min(d, n_ang - d), d))
    barrier = pltpu.get_barrier_semaphore()
    angle_peers = [lax.rem(me_a + d, n_ang) for d in order]
    pos_peers = [lax.rem(me_p + d, n_pos) for d in range(1, n_pos)]
    for peer in angle_peers:
        pl.semaphore_signal(barrier, inc=1, device_id={"angle": peer}, device_id_type=MESH)
    for peer in pos_peers:
        pl.semaphore_signal(barrier, inc=1, device_id={"pos": peer}, device_id_type=MESH)
    own = pltpu.make_async_copy(new_obj.at[0, 1, pl.ds(pl.multiple_of(me_a * ns, 8), ns), :],
                                sino.at[me_a], local_sem.at[0])
    own.start()
    sources = [me_a] + [lax.rem(me_a + n_ang - d, n_ang) for d in order]
    loads = []
    for k, a in enumerate(sources):
        span = pl.ds(a * per_angle, per_angle)
        loads.append(pltpu.make_async_copy(onehot.at[span], tables.at[span], table_sem.at[k]))
    loads[0].start()
    pl.semaphore_wait(barrier, n_ang + n_pos - 2)
    gather = [
        remote(partial, ag.at[me_a], ag_send.at[k], ag_recv.at[k], "angle", peer)
        for k, peer in enumerate(angle_peers)
    ]
    for copy in gather:
        copy.start()
    across = [
        remote(new_obj.at[0, 1, pl.ds(pl.multiple_of(peer * ns, 8), ns), :], sino.at[me_a],
               a2a_send.at[k], a2a_recv.at[k], "angle", peer)
        for k, peer in enumerate(angle_peers)
    ]
    for copy in across:
        copy.start()
    for copy in loads[1:]:
        copy.start()
    tall = 64

    def ramp(step, carry):
        top = pl.multiple_of(step * tall, tall)
        shape = (tall, width)
        differ = lax.broadcasted_iota(jnp.int32, shape, 1) - (
            lax.broadcasted_iota(jnp.int32, shape, 0) + top)
        spread = differ.astype(jnp.float32)
        odd = -1.0 / (jnp.maximum(spread * spread, 1.0) * (math.pi * math.pi))
        value = jnp.where((differ & 1) == 1, odd, jnp.where(differ == 0, 0.25, 0.0))
        rh[pl.ds(top, tall), :], rl[pl.ds(top, tall), :] = halves(value)
        return carry

    lax.fori_loop(0, width // tall, ramp, 0)

    def project(k):
        a = sources[k]
        high, low = halves(sino[a])
        both = mm(jnp.concatenate([high, low], axis=0), rh[...])
        lines = (both[:ns] + both[ns:] + mm(high, rl[...])) * (math.pi / n_ang)
        high, low = halves(lines)
        next_high, next_low = halves(pltpu.roll(lines, width - 1, 1))
        stack = jnp.concatenate([high, low, next_high, next_low], axis=0)
        loads[k].wait()
        for n in range(per_angle):
            z, part = n // per_row, n % per_row
            got = mm(stack, tables[a * per_angle + n])
            lower = got[:ns] + got[ns:2 * ns]
            upper = got[2 * ns:3 * ns] + got[3 * ns:]
            w = weight[pl.ds(a, 1), z, pl.ds(part * chunk, chunk)]
            value = (1.0 - w) * lower + w * upper
            lanes = pl.ds(n * chunk, chunk)
            recon[:, lanes] = value if k == 0 else recon[:, lanes] + value

    ag[me_a] = partial[...]
    for copy in gather:
        copy.wait()
    mine = pl.ds(pl.multiple_of(me_p * pr, 8), pr)
    whole = ag[0]
    for a in range(1, n_ang):
        whole = whole + ag[a]
    for c in range(2):
        value = whole[c] / (whole[2] + 1.0)
        piece[c] = value
        newp[c, mine, :] = value
    spread = [
        remote(piece, newp.at[:, mine, :], fin_send.at[d], fin_recv.at[d], "pos", peer)
        for d, peer in enumerate(pos_peers)
    ]
    for copy in spread:
        copy.start()
    own.wait()
    project(0)
    for k in range(1, n_ang):
        across[k - 1].wait()
        project(k)
    for copy in spread:
        copy.wait()


def on_device(n_ang, n_pos, amplitude, offsets, probe_field, object_field, interp_index, interp_weight):
    band = object_field.shape[2]
    width = object_field.shape[3]
    patch = probe_field.shape[1]
    half = patch // 2
    count = offsets.shape[1]
    f32, i32 = jnp.float32, jnp.int32
    start = lax.axis_index("pos").astype(i32) * band
    own = offsets[0]
    corner = own.T - jnp.where(jnp.arange(2)[:, None] == 0, start - half, 0)
    where_at = corner[::-1, :, None] + jnp.arange(patch, dtype=i32)[None, None, :]
    where_at = where_at.reshape(2, count * patch)
    padded = jnp.pad(own.reshape(1, 2 * count), ((0, 7), (0, 128 - 2 * count)))
    n_z = interp_index.shape[1]
    chunk = min(512, width)
    tables = n_ang * n_z * (width // chunk)
    bf16 = jnp.bfloat16
    left, right = dft_blocks(patch)
    ah, al = split_const(left)
    bh, bl = split_const(right)
    vmem = pl.BlockSpec(memory_space=VMEM)
    smem = pl.BlockSpec(memory_space=pltpu.SMEM)
    hbm = pl.BlockSpec(memory_space=pl.ANY)
    sds = jax.ShapeDtypeStruct
    dma = pltpu.SemaphoreType.DMA
    half_shape = (count, 2, half, patch)
    grad, from_above, from_below, near, partial, onehot = pl.pallas_call(
        functools.partial(patch_kernel, n_pos),
        out_shape=(
            sds((2,) + half_shape, f32), sds(half_shape, f32), sds(half_shape, f32),
            sds((2, 8, 128), i32), sds((3, patch // n_pos, patch), f32),
            sds((tables, width, chunk), bf16),
        ),
        in_specs=[vmem, hbm] + [vmem] * 8,
        out_specs=(vmem,) * 5 + (hbm,),
        scratch_shapes=[
            VMEM((2, band + patch, width), f32),
            VMEM((2, width, chunk), bf16),
            VMEM((3, patch, patch), f32),
            VMEM((n_pos - 1, 3, patch // n_pos, patch), f32),
            dma((1,)), dma((2,)), dma((4 + 2 * count,)), dma((4 + 2 * count,)), dma((n_pos - 1,)), dma((n_pos - 1,)),
        ],
        compiler_params=pltpu.CompilerParams(collective_id=0, has_side_effects=True),
        name="patches",
    )(where_at, object_field, padded, interp_index, amplitude[0], probe_field, ah, al, bh, bl)
    new_object = pl.pallas_call(
        functools.partial(merge_kernel, count),
        out_shape=sds(object_field.shape, f32),
        in_specs=[smem] * 3 + [vmem] * 5,
        out_specs=vmem,
        scratch_shapes=[VMEM((3, band + 2 * patch + 8, width), f32)],
        name="merge",
    )(start[None], padded, near, object_field, probe_field, grad, from_above, from_below)
    total = n_z * width
    ns = band // n_ang
    pr = patch // n_pos
    recon, change = pl.pallas_call(
        functools.partial(final_kernel, n_ang, n_pos),
        out_shape=(sds((ns, total), f32), sds(probe_field.shape, f32)),
        in_specs=[hbm] + [vmem] * 2 + [hbm],
        out_specs=(vmem, vmem),
        scratch_shapes=[
            VMEM((n_ang, ns, width), f32),
            VMEM((tables, width, chunk), bf16),
            VMEM((width, width), bf16), VMEM((width, width), bf16),
            VMEM((n_ang, 3, pr, patch), f32),
            VMEM((2, pr, patch), f32),
            dma((1,)), dma((n_ang,)),
            dma((n_ang - 1,)), dma((n_ang - 1,)),
            dma((n_ang - 1,)), dma((n_ang - 1,)),
            dma((n_pos - 1,)), dma((n_pos - 1,)),
        ],
        compiler_params=pltpu.CompilerParams(
            collective_id=1, has_side_effects=True, vmem_limit_bytes=BIG),
        name="final",
    )(new_object, partial, interp_weight, onehot)
    return new_object, probe_field + change, recon.reshape(1, ns, n_z, width)


def solution(mesh):
    placed = (
        P("angle", "pos", None, None),
        P("angle", "pos", None),
        P(),
        P("angle", None, "pos", None),
        P(),
        P(),
    )
    return jax.shard_map(
        functools.partial(on_device, mesh.shape["angle"], mesh.shape["pos"]),
        mesh=mesh,
        in_specs=placed,
        out_specs=(P("angle", None, "pos", None), P(), P("pos", "angle", None, None)),
        check_vma=False,
    )
```
